8 devices in a mesh: dp: 2 (over z, y), tp: 4 (over x, core).
Axes of the slice: x: 2, y: 2, z: 1, core: 2. Of those that a mesh axis runs over, the one named last changes fastest.
Arguments:
- x: bfloat16 [2, 2048, 2560], P('dp', 'tp'), parts along dimension 0
- ln_gain: bfloat16 [2, 2560], replicated
- ln_bias: bfloat16 [2, 2560], replicated
- w_q: bfloat16 [2, 2560, 32, 80], P(None, None, 'tp')
- b_q: bfloat16 [2, 32, 80], P(None, 'tp')
- w_k: bfloat16 [2, 2560, 32, 80], P(None, None, 'tp')
- b_k: bfloat16 [2, 32, 80], P(None, 'tp')
- w_v: bfloat16 [2, 2560, 32, 80], P(None, None, 'tp')
- b_v: bfloat16 [2, 32, 80], P(None, 'tp')
- w_o: bfloat16 [2, 32, 80, 2560], P(None, 'tp')
- b_o: bfloat16 [2, 2560], replicated
- w_up: bfloat16 [2, 2560, 10240], P(None, None, 'tp')
- b_up: bfloat16 [2, 10240], P(None, 'tp')
- w_down: bfloat16 [2, 10240, 2560], P(None, 'tp')
- b_down: bfloat16 [2, 2560], replicated
Outputs:
- output: bfloat16 [2, 2048, 2560], P('dp', 'tp'), parts along dimension 0
There are 2 independent parts. The reference program is written for one: setup_inputs(seed, part) draws one part's arguments, and reference() takes and returns one part's arrays. A program takes and returns all parts, laid end to end along the dimension named above; an argument that names none is the same for every part.
All inputs are finite; a program needn't handle non-finite values.
Results may differ from the reference program's by a relative error of at most 0.0153974.
Values are sent between devices in bfloat16 or wider.
A program may use at most 1 GiB of HBM per device.

```python
import jax
import jax.numpy as jnp
from jax import lax

N_BATCH = 1
SEQ_LEN = 2048
D_MODEL = 2560
N_HEADS = 32
HEAD_DIM = 80
D_FF = 10240
ROT_DIM = 32
N_LAYERS = 2


def setup_inputs(seed: int = 0, part: int = 0) -> dict:
    shared_keys = jax.random.split(jax.random.key(seed), 14)
    token_key = jax.random.fold_in(jax.random.key(seed + 1), part)

    def draw(key_index, shape, scale, offset):
        sample = jax.random.normal(shared_keys[key_index], shape, jnp.float32)
        return (offset + scale * sample).astype(jnp.bfloat16)

    proj_shape = (N_LAYERS, D_MODEL, N_HEADS, HEAD_DIM)
    head_shape = (N_LAYERS, N_HEADS, HEAD_DIM)
    wide_shape = (N_LAYERS, D_MODEL)
    in_scale = D_MODEL ** -0.5
    x = jax.random.normal(token_key, (N_BATCH, SEQ_LEN, D_MODEL), jnp.float32).astype(jnp.bfloat16)
    return {
        "x": x,
        "ln_gain": draw(0, wide_shape, 0.3, 1.0),
        "ln_bias": draw(1, wide_shape, 0.3, 0.0),
        "w_q": draw(2, proj_shape, 2.0 * in_scale, 0.0),
        "b_q": draw(3, head_shape, 0.5, 0.0),
        "w_k": draw(4, proj_shape, 2.0 * in_scale, 0.0),
        "b_k": draw(5, head_shape, 0.5, 0.0),
        "w_v": draw(6, proj_shape, in_scale, 0.0),
        "b_v": draw(7, head_shape, 0.5, 0.0),
        "w_o": draw(8, (N_LAYERS, N_HEADS, HEAD_DIM, D_MODEL), in_scale, 0.0),
        "b_o": draw(9, wide_shape, 0.5, 0.0),
        "w_up": draw(10, (N_LAYERS, D_MODEL, D_FF), in_scale, 0.0),
        "b_up": draw(11, (N_LAYERS, D_FF), 0.5, 0.0),
        "w_down": draw(12, (N_LAYERS, D_FF, D_MODEL), D_FF ** -0.5, 0.0),
        "b_down": draw(13, wide_shape, 0.5, 0.0),
    }


def rotary_tables():
    half = ROT_DIM // 2
    inv_freq = 1.0 / (10000.0 ** (jnp.arange(half, dtype=jnp.float32) * (2.0 / ROT_DIM)))
    angles = jnp.arange(SEQ_LEN, dtype=jnp.float32)[:, None] * inv_freq[None, :]
    return jnp.cos(angles)[:, None, :], jnp.sin(angles)[:, None, :]


def apply_rotary(projected, cosine, sine):
    half = ROT_DIM // 2
    first = projected[..., :half]
    second = projected[..., half:ROT_DIM]
    return jnp.concatenate([first * cosine - second * sine, second * cosine + first * sine, projected[..., ROT_DIM:]], axis=-1)


def attend_heads(q_rot, k_rot, values):
    def per_head(operands):
        q_one, k_one, v_one = operands
        scores = jnp.dot(q_one, jnp.transpose(k_one), preferred_element_type=jnp.float32) * (HEAD_DIM ** -0.5)
        causal = jnp.arange(SEQ_LEN)[:, None] >= jnp.arange(SEQ_LEN)[None, :]
        attn_probs = jax.nn.softmax(jnp.where(causal, scores, -1e30), axis=-1).astype(jnp.bfloat16)
        return jnp.dot(attn_probs, v_one, preferred_element_type=jnp.float32).astype(jnp.bfloat16)

    def by_head(tensor):
        return jnp.transpose(tensor, (0, 2, 1, 3)).reshape(N_BATCH * N_HEADS, SEQ_LEN, HEAD_DIM)

    head_out = lax.map(per_head, (by_head(q_rot), by_head(k_rot), by_head(values)))
    return jnp.transpose(head_out.reshape(N_BATCH, N_HEADS, SEQ_LEN, HEAD_DIM), (0, 2, 1, 3))


def layer_forward(hidden, layer_params):
    (ln_gain, ln_bias, w_q, b_q, w_k, b_k, w_v, b_v, w_o, b_o, w_up, b_up, w_down, b_down) = layer_params
    x_f32 = hidden.astype(jnp.float32)
    mean = jnp.mean(x_f32, axis=-1, keepdims=True)
    centered = x_f32 - mean
    variance = jnp.mean(centered * centered, axis=-1, keepdims=True)
    normed = (centered * lax.rsqrt(variance + 1e-5) * ln_gain.astype(jnp.float32) + ln_bias.astype(jnp.float32)).astype(jnp.bfloat16)
    flat = normed.reshape(N_BATCH * SEQ_LEN, D_MODEL)
    head_shape = (N_BATCH, SEQ_LEN, N_HEADS, HEAD_DIM)
    cosine, sine = rotary_tables()

    def project(weight, bias):
        prod = jnp.dot(flat, weight.reshape(D_MODEL, N_HEADS * HEAD_DIM), preferred_element_type=jnp.float32)
        return prod.reshape(head_shape) + bias.astype(jnp.float32)

    q_rot = apply_rotary(project(w_q, b_q), cosine, sine).astype(jnp.bfloat16)
    k_rot = apply_rotary(project(w_k, b_k), cosine, sine).astype(jnp.bfloat16)
    values = project(w_v, b_v).astype(jnp.bfloat16)
    attended = attend_heads(q_rot, k_rot, values)
    dense_out = jnp.dot(attended.reshape(N_BATCH * SEQ_LEN, D_MODEL), w_o.reshape(D_MODEL, D_MODEL), preferred_element_type=jnp.float32)
    up_act = jax.nn.gelu(jnp.dot(flat, w_up, preferred_element_type=jnp.float32) + b_up.astype(jnp.float32), approximate=True).astype(jnp.bfloat16)
    down_out = jnp.dot(up_act, w_down, preferred_element_type=jnp.float32)
    total = x_f32.reshape(N_BATCH * SEQ_LEN, D_MODEL) + dense_out + down_out + b_o.astype(jnp.float32) + b_down.astype(jnp.float32)
    return total.reshape(N_BATCH, SEQ_LEN, D_MODEL).astype(jnp.bfloat16)


def reference(x, ln_gain, ln_bias, w_q, b_q, w_k, b_k, w_v, b_v, w_o, b_o, w_up, b_up, w_down, b_down):
    stacked = (ln_gain, ln_bias, w_q, b_q, w_k, b_k, w_v, b_v, w_o, b_o, w_up, b_up, w_down, b_down)

    def layer_body(hidden, layer_params):
        return layer_forward(hidden, layer_params), None

    final = lax.scan(layer_body, x, stacked)
    return final[0]
```

```python
import functools

import jax
import jax.numpy as jnp
import numpy as np
from jax import lax
from jax.experimental import pallas as pl
from jax.experimental.pallas import tpu as pltpu
from jax.sharding import PartitionSpec as P


F32, BF16 = jnp.float32, jnp.bfloat16
ROT_DIM = 32
UNIT = ROT_DIM // 2
ROPE_BASE = 10000.0
LN_EPS = 1e-5
LANES = 128
VMEM_LIMIT = 60 * 2**20
ROWS = 512
HEADS = 8
HEAD_DIM = 80
PAIRS = HEADS // 2
ANY = pl.BlockSpec(memory_space=pl.ANY)
VM = pl.BlockSpec(memory_space=pltpu.VMEM)


def packed_units():
    cols = [[None] * 8 for _ in range(5)]
    rest = []
    for p in range(PAIRS):
        base = 2 * (p % 2)
        for e in range(2):
            head = 2 * p + e
            cols[p][base + e] = (head, 0)
            cols[p + 1][base + e] = (head, 1)
    in_first = (6, 4, 2, 0)
    for p in range(PAIRS):
        units = [(2 * p + e, 2 + i) for e in range(2) for i in range(3)]
        rest.append((p, units[:in_first[p]], units[in_first[p]:]))
    for p, first, second in rest:
        for col, units in ((p, first), (p + 1, second)):
            for u in units:
                cols[col][cols[col].index(None)] = u
    return [u for col in cols for u in col]


UNITS = packed_units()
UNIT_ROWS = [h * HEAD_DIM + u * UNIT for h, u in UNITS]


def unit_runs():
    runs, start = [], 0
    for i in range(1, len(UNIT_ROWS) + 1):
        if i == len(UNIT_ROWS) or UNIT_ROWS[i] != UNIT_ROWS[i - 1] + UNIT:
            runs.append((UNIT_ROWS[start], start * UNIT, (i - start) * UNIT))
            start = i
    return runs


def head_masks():
    qk = np.zeros((HEADS, 1, 2 * LANES), np.float32)
    ov = np.zeros((HEADS, 1, 2 * LANES), np.float32)
    for i, (h, _) in enumerate(UNITS):
        lane = i * UNIT - (h // 2) * LANES
        qk[h, 0, lane:lane + UNIT] = 1.0
    for h in range(HEADS):
        lane = h * HEAD_DIM - (h // 2) * LANES
        ov[h, 0, lane:lane + HEAD_DIM] = 1.0
    return qk, ov


def gelu(x):
    return 0.5 * x * (1.0 + jnp.tanh(0.7978845608028654 * (x + 0.044715 * (x * x * x))))


def pre_kernel(nf, layer, n_pair, n_after, info, *refs):
    x_hbm, refs = refs[:2 * n_pair], refs[2 * n_pair:]
    (wq, wk, wv, bqkv_ref, cos_hbm, sin_hbm, wu, bu_ref, wd), refs = refs[:9], refs[9 + n_after:]
    q_out, k_out, v_out, mlp_out = refs[:4]
    x_s, tab_s, y_s, h_s, z_s, u_s, o_s, wp_s, wt_s, x_sem, p_sem, t_sem, h_sem, o_sem = refs[4:]
    R, _ = x_s.shape
    half = ROWS // 2
    nr = R // ROWS
    bf = wt_s.shape[2]
    N = HEADS * HEAD_DIM
    block, core = info[0], info[1]
    row0 = pl.multiple_of(core * half, half)
    row1 = pl.multiple_of((1 - core) * half, half)
    brow = pl.multiple_of(block * ROWS, ROWS)
    xcopies = []
    for p in range(n_pair):
        for s, row in enumerate((row0, row1)):
            xcopies.append(pltpu.make_async_copy(x_hbm[2 * p + s], x_s.at[pl.ds(p * ROWS + row, half)], x_sem.at[2 * p + s]))
    tcopies = [pltpu.make_async_copy(t.at[pl.ds(brow, R)], tab_s.at[s], x_sem.at[2 * n_pair + s]) for s, t in enumerate((cos_hbm, sin_hbm))]
    pcopies = []
    for s, w in enumerate((wq, wk)):
        for src, dst, n in unit_runs():
            pcopies.append(pltpu.make_async_copy(w.at[layer, pl.ds(src, n)], wp_s.at[pl.ds(s * N + dst, n)], p_sem.at[s]))
    pcopies.append(pltpu.make_async_copy(wv.at[layer], wp_s.at[pl.ds(2 * N, N)], p_sem.at[2]))
    pwaits = [pltpu.make_async_copy(w.at[layer], wp_s.at[pl.ds(s * N, N)], p_sem.at[s]) for s, w in enumerate((wq, wk, wv))]
    kv_rows = pl.ds(brow, R)
    hcopies = [pltpu.make_async_copy(h_s.at[0], q_out, h_sem.at[0]),
               pltpu.make_async_copy(h_s.at[1], k_out.at[kv_rows], h_sem.at[1]),
               pltpu.make_async_copy(h_s.at[2], v_out.at[kv_rows], h_sem.at[2])]

    def tile_copy(w, t, slot):
        return pltpu.make_async_copy(w.at[layer, :, pl.ds(pl.multiple_of(t * bf, bf), bf)], wt_s.at[slot], t_sem.at[slot])

    def out_copy(t):
        slot = lax.rem(t, 2)
        return pltpu.make_async_copy(o_s.at[slot], mlp_out.at[:, pl.ds(pl.multiple_of(t * bf, bf), bf)], o_sem.at[slot])

    def epilogue(r):
        step = 64
        lane = lax.broadcasted_iota(jnp.int32, (step, LANES), 1)
        low, mid = lane < 2 * UNIT, lane < 4 * UNIT
        high = jnp.logical_and(mid, jnp.logical_not(low))
        for rr in range(r * ROWS, (r + 1) * ROWS, step):
            rows = slice(rr, rr + step)
            cos, sin = tab_s[0, rows, :], tab_s[1, rows, :]
            cos_a, cos_ab, cos_b = jnp.where(low, cos, 1.0), jnp.where(mid, cos, 1.0), jnp.where(high, cos, 1.0)
            sin_a, sin_b = jnp.where(low, sin, 0.0), jnp.where(high, sin, 0.0)
            for s in range(3):
                c = [y_s[rows, s * N + i * LANES:s * N + (i + 1) * LANES] + bqkv_ref[:, s * N + i * LANES:s * N + (i + 1) * LANES] for i in range(5)]
                if s < 2:
                    c = [c[0] * cos_a - c[1] * sin_a,
                         c[1] * cos_ab + c[0] * sin_a - c[2] * sin_b,
                         c[2] * cos_ab + c[1] * sin_b - c[3] * sin_a,
                         c[3] * cos_ab + c[2] * sin_a - c[4] * sin_b,
                         c[4] * cos_b + c[3] * sin_b]
                for i in range(5):
                    h_s[s, rows, i * LANES:(i + 1) * LANES] = c[i].astype(BF16)

    def activate(t):
        step = 64
        slot = lax.rem(t, 2)
        bias = bu_ref[t].astype(F32)
        for rr in range(0, R, step):
            u_s[t + 1, rr:rr + step, :] = gelu(z_s[slot, rr:rr + step, :] + bias).astype(BF16)

    def slot3(t):
        return lax.rem(t, 3)

    for cp in xcopies:
        cp.start()
    tile_copy(wu, 0, 0).start()
    tile_copy(wu, 1, 1).start()
    for cp in pcopies + tcopies:
        cp.start()
    for cp in xcopies:
        cp.wait()

    def up_tile(t, first):
        tile_copy(wu, t, slot3(t)).wait()
        if isinstance(t, int):
            (tile_copy(wu, t + 2, slot3(t + 2)) if t + 2 < nf else tile_copy(wd, t + 2 - nf, slot3(t + 2))).start()
        else:
            @pl.when(t + 2 < nf)
            def _():
                tile_copy(wu, t + 2, slot3(t + 2)).start()

            @pl.when(t + 2 >= nf)
            def _():
                tile_copy(wd, t + 2 - nf, slot3(t + 2)).start()
        z_s[lax.rem(t, 2)] = jnp.dot(x_s[...], wt_s[slot3(t)], preferred_element_type=F32)
        if not first:
            activate(t - 1)

    if nr == 1:
        for t in range(nf):
            up_tile(t, t == 0)
    else:
        up_tile(0, True)
        lax.fori_loop(1, nf, lambda t, c: (up_tile(t, False), c)[1], 0)
    for cp in pwaits + tcopies:
        cp.wait()
    for r in range(nr):
        rows = slice(r * ROWS, (r + 1) * ROWS)
        y_s[rows, :] = lax.dot_general(x_s[rows, :], wp_s[...], (((1,), (1,)), ((), ())), preferred_element_type=F32)
        if r == 0:
            activate(nf - 1)
        else:
            epilogue(r - 1)

    def down_tile(t, first):
        slot = slot3(t + nf)
        tile_copy(wd, t, slot).wait()
        if isinstance(t, int):
            if t + 2 < nf:
                tile_copy(wd, t + 2, slot3(t + nf + 2)).start()
            if t >= 2:
                out_copy(t - 2).wait()
        else:
            @pl.when(t + 2 < nf)
            def _():
                tile_copy(wd, t + 2, slot3(t + nf + 2)).start()

            @pl.when(t >= 2)
            def _():
                out_copy(t - 2).wait()
        u = jnp.concatenate([u_s[f + 1] for f in range(nf)], axis=1)
        o = jnp.dot(u, wt_s[slot], preferred_element_type=F32)
        if first:
            epilogue(nr - 1)
        o_s[lax.rem(t, 2)] = o.astype(BF16)
        out_copy(t).start()
        if first:
            for cp in hcopies:
                cp.start()

    if nr == 1:
        for t in range(nf):
            down_tile(t, t == 0)
    else:
        down_tile(0, True)
        lax.fori_loop(1, nf, lambda t, c: (down_tile(t, False), c)[1], 0)
    out_copy(nf - 2).wait()
    out_copy(nf - 1).wait()
    for cp in hcopies:
        cp.wait()


def pre(layer, info, xs, wq, wk, wv, b_qkv, cos_t, sin_t, w_up, b_up, w_down, kg, vg, after, L, bf=512):
    half, D = xs[0].shape
    n_pair = len(xs) // 2
    R = n_pair * 2 * half
    F = w_up.shape[2]
    nf = F // bf
    N = HEADS * HEAD_DIM
    after = list(after)
    chain = [] if kg is None else [kg, vg]
    n0 = 1 + len(xs) + 9 + len(after)
    return pl.pallas_call(
        functools.partial(pre_kernel, nf, layer, n_pair, len(after) + len(chain)),
        grid_spec=pltpu.PrefetchScalarGridSpec(
            num_scalar_prefetch=1, grid=(),
            in_specs=[ANY] * (len(xs) + 3) + [VM, ANY, ANY, ANY, VM, ANY] + [ANY] * (len(after) + len(chain)),
            out_specs=[ANY] * 4,
            scratch_shapes=[pltpu.VMEM((R, D), BF16), pltpu.VMEM((2, R, LANES), F32), pltpu.VMEM((R, 3 * N), F32),
                            pltpu.VMEM((3, R, N), BF16), pltpu.VMEM((2, R, bf), F32), pltpu.VMEM((nf + 1, R, bf), BF16),
                            pltpu.VMEM((2, R, bf), BF16), pltpu.VMEM((3 * N, D), BF16), pltpu.VMEM((3, D, bf), BF16),
                            pltpu.SemaphoreType.DMA((2 * n_pair + 2,)), pltpu.SemaphoreType.DMA((3,)), pltpu.SemaphoreType.DMA((3,)),
                            pltpu.SemaphoreType.DMA((3,)), pltpu.SemaphoreType.DMA((2,))]),
        out_shape=[jax.ShapeDtypeStruct((R, N), BF16)] + [jax.ShapeDtypeStruct((L, N), BF16)] * 2 + [jax.ShapeDtypeStruct((R, D), BF16)],
        input_output_aliases={} if kg is None else {n0: 1, n0 + 1: 2}, name="pre",
        compiler_params=pltpu.CompilerParams(vmem_limit_bytes=VMEM_LIMIT),
        cost_estimate=pl.CostEstimate(flops=4 * R * D * F + 6 * R * D * N, bytes_accessed=4 * D * F + 4 * R * D, transcendentals=R * F),
    )(info, *xs, wq, wk, wv, b_qkv, cos_t, sin_t, w_up, b_up, w_down, *after, *chain)


def attn_kernel(layer, bases, n_blocks, n_after, info, qm_ref, om_ref, k_hbm, v_hbm, wo_hbm, *refs):
    q_hbm, mlp_hbm, refs = refs[:n_blocks], refs[n_blocks:2 * n_blocks], refs[2 * n_blocks:]
    mine_out, part_out, q_s, k_s, v_s, o_s, m_s, w_s, r_s, in_sem, w_sem, out_sem = refs[n_after:]
    R = q_s.shape[0]
    half = ROWS // 2
    n_blk = R // half
    scale = (HEAD_DIM ** -0.5) * 1.4426950408889634
    cp_w = pltpu.make_async_copy(wo_hbm.at[layer], w_s, w_sem.at[0])
    cp_m = [pltpu.make_async_copy(m, m_s.at[pl.ds(i * ROWS, ROWS)], w_sem.at[1 + i]) for i, m in enumerate(mlp_hbm)]
    cp_in = [pltpu.make_async_copy(src, dst, in_sem.at[i]) for i, (src, dst) in enumerate(((k_hbm, k_s), (v_hbm, v_s)))]
    cp_in += [pltpu.make_async_copy(q, q_s.at[pl.ds(i * ROWS, ROWS)], in_sem.at[2 + i]) for i, q in enumerate(q_hbm)]
    for cp in cp_in:
        cp.start()
    cp_w.start()
    for cp in cp_m:
        cp.start()
    o_s[...] = jnp.zeros_like(o_s)
    for cp in cp_in:
        cp.wait()

    def run(base):
        def pair(p, carry):
            lanes = pl.ds(pl.multiple_of(p * LANES, LANES), 2 * LANES)
            tasks = [(e, i) for i in range(n_blk) for e in range(2)]

            def scores(e, i):
                n = base + (i + 1) * half
                q = q_s[i * half:(i + 1) * half, lanes] * qm_ref[2 * p + e]
                return lax.dot_general(q, k_s[:n, lanes], (((1,), (1,)), ((), ())), preferred_element_type=F32)

            def rest(s, e, i):
                n = base + (i + 1) * half
                row = lax.broadcasted_iota(jnp.int32, (half, half), 0)
                col = lax.broadcasted_iota(jnp.int32, (half, half), 1)
                diag = jnp.where(row >= col, s[:, n - half:], -1e30)
                s = jnp.concatenate([s[:, :n - half], diag], axis=1) if n > half else diag
                m = jnp.max(s, axis=1, keepdims=True)
                prob = jnp.exp2((s - m) * scale)
                den = jnp.sum(prob, axis=1, keepdims=True)
                o = jnp.dot(prob.astype(BF16), v_s[:n, lanes], preferred_element_type=F32)
                o = jnp.where(om_ref[2 * p + e] > 0.5, o * (1.0 / den), 0.0)
                rows = slice(i * half, (i + 1) * half)
                o_s[rows, lanes] = o_s[rows, lanes] + o.astype(BF16)

            s = scores(*tasks[0])
            for a, t in enumerate(tasks):
                nxt = scores(*tasks[a + 1]) if a + 1 < len(tasks) else None
                rest(s, *t)
                s = nxt
            return carry

        lax.fori_loop(0, PAIRS, pair, 0)

    @pl.when(info[0] < 2)
    def _():
        run(bases[0])

    @pl.when(info[0] >= 2)
    def _():
        run(bases[1])

    cp_w.wait()
    for cp in cp_m:
        cp.wait()
    core = info[1]
    copies = []
    for i in range(n_blk):
        rows = slice(i * half, (i + 1) * half)
        r_s[rows, :] = (jnp.dot(o_s[rows, :], w_s[...], preferred_element_type=F32) + m_s[rows, :].astype(F32)).astype(BF16)
        if i % 2 == 1:
            p = i // 2
            for s, (ref, hf) in enumerate(((mine_out, core), (part_out, 1 - core))):
                cp = pltpu.make_async_copy(r_s.at[pl.ds(pl.multiple_of(p * ROWS + hf * half, half), half)], ref.at[pl.ds(p * half, half)], out_sem.at[2 * p + s])
                cp.start()
                copies.append(cp)
    for cp in copies:
        cp.wait()


def attn(layer, bases, info, masks, q, kg, vg, mlp_part, w_o, after=()):
    n_blocks, N = len(q), q[0].shape[1]
    R = n_blocks * ROWS
    L = kg.shape[0]
    D = w_o.shape[2]
    after = list(after)
    return pl.pallas_call(
        functools.partial(attn_kernel, layer, bases, n_blocks, len(after)),
        grid_spec=pltpu.PrefetchScalarGridSpec(
            num_scalar_prefetch=1, grid=(),
            in_specs=[VM, VM] + [ANY] * (3 + 2 * n_blocks + len(after)),
            out_specs=[ANY, ANY],
            scratch_shapes=[pltpu.VMEM((R, N), BF16), pltpu.VMEM((L, N), BF16), pltpu.VMEM((L, N), BF16), pltpu.VMEM((R, N), BF16),
                            pltpu.VMEM((R, D), BF16), pltpu.VMEM((N, D), BF16), pltpu.VMEM((R, D), BF16),
                            pltpu.SemaphoreType.DMA((2 + n_blocks,)), pltpu.SemaphoreType.DMA((1 + n_blocks,)), pltpu.SemaphoreType.DMA((2 * n_blocks,))]),
        out_shape=[jax.ShapeDtypeStruct((R // 2, D), BF16)] * 2, name="attn",
        compiler_params=pltpu.CompilerParams(vmem_limit_bytes=VMEM_LIMIT),
        cost_estimate=pl.CostEstimate(flops=4 * HEADS * R * (L // 2) * 128 + 2 * R * D * N, bytes_accessed=4 * L * N, transcendentals=HEADS * R * L // 2),
    )(info, *masks, kg, vg, w_o, *q, *mlp_part, *after)


def rotary_tables(seq_len):
    inv_freq = 1.0 / (ROPE_BASE ** (jnp.arange(UNIT, dtype=F32) * (2.0 / ROT_DIM)))
    angles = jnp.arange(seq_len, dtype=F32)[:, None] * inv_freq[None, :]
    return jnp.tile(jnp.cos(angles), (1, LANES // UNIT)), jnp.tile(jnp.sin(angles), (1, LANES // UNIT))


def layer_norm(x_f32, gain, bias):
    mean = jnp.mean(x_f32, axis=-1, keepdims=True)
    centered = x_f32 - mean
    variance = jnp.mean(centered * centered, axis=-1, keepdims=True)
    return (centered * lax.rsqrt(variance + LN_EPS) * gain.astype(F32) + bias.astype(F32)).astype(BF16)


def solution(mesh):
    head_spec = P(None, None, "tp", None)
    head_bias_spec = P(None, "tp", None)
    in_specs = (P("dp", "tp", None), P(), P(), head_spec, head_bias_spec, head_spec, head_bias_spec, head_spec, head_bias_spec,
                P(None, "tp", None, None), P(), P(None, None, "tp"), P(None, "tp"), P(None, "tp", None), P())
    across = [(0, 2), (1, 3), (2, 0), (3, 1)]
    partner = [(0, 1), (1, 0), (2, 3), (3, 2)]

    def to_chip(a):
        return lax.ppermute(a, "tp", across)

    def to_core(a):
        return lax.ppermute(a, "tp", partner)

    def behind(a, done):
        return lax.optimization_barrier((a, done))[0]

    def local_program(x_loc, ln_gain, ln_bias, w_q, b_q, w_k, b_k, w_v, b_v, w_o, b_o, w_up, b_up, w_down, b_down):
        n_layers, d_model, heads, head_dim = w_q.shape
        width = heads * head_dim
        half = x_loc.shape[1] // 2
        seq_len = 4 * x_loc.shape[1]
        index = lax.axis_index("tp")
        chip, core = index // 2, index % 2
        cos_t, sin_t = rotary_tables(seq_len)
        qk_mask, out_mask = head_masks()
        masks = (jnp.asarray(qk_mask, BF16), jnp.asarray(out_mask, F32))
        w_o2 = w_o.reshape(n_layers, width, d_model)
        w_qt, w_kt, w_vt = (jnp.transpose(w, (0, 2, 3, 1)).reshape(n_layers, width, d_model) for w in (w_q, w_k, w_v))

        def pick(first, second):
            return jnp.where(core == 0, first, second)

        def packed(bias):
            flat = bias.astype(F32).reshape(width)
            return jnp.concatenate([flat[r:r + UNIT] for r in UNIT_ROWS])

        x_halves = x_loc[0, :half], x_loc[0, half:]
        keep = pick(*x_halves)
        recv = to_core(pick(x_halves[1], x_halves[0]))
        res = [pick(keep, recv), pick(recv, keep)]
        info_own = [jnp.stack([2 * chip + j, core]).astype(jnp.int32) for j in range(2)]
        info_oth = [jnp.stack([2 * (1 - chip) + j, core]).astype(jnp.int32) for j in range(2)]

        def run_layer(layer, res):
            b_qkv = jnp.concatenate([packed(b_q[layer]), packed(b_k[layer]), b_v[layer].astype(F32).reshape(width)])[None]
            b_up3 = b_up[layer].reshape(-1, 1, 512)
            norm = [layer_norm(res[j].astype(F32), ln_gain[layer], ln_bias[layer]) for j in range(2)]
            far = [None, None]
            for j in range(2):
                far[j] = to_chip(norm[j])
            near = [to_core(norm[j]) for j in range(2)]

            def project(info, a, b, kg, vg, after):
                return pre(layer, info, [a, b], w_qt, w_kt, w_vt, b_qkv, cos_t, sin_t, w_up, b_up3, w_down, kg, vg, after, seq_len)

            q_own, mlp_own, relay = [None, None], [None, None], [None, None]
            kg = vg = None
            after = []
            for j in range(2):
                q_own[j], kg, vg, mlp_own[j] = project(info_own[j], norm[j], near[j], kg, vg, after)
                far[j] = behind(far[j], mlp_own[j])
                relay[j] = to_core(far[j])
                after = [far[j]]
            arrived = [None, None]
            for j in range(2):
                q_oth, kg, vg, mlp_oth = project(info_oth[j], far[j], relay[j], kg, vg, after)
                mine, other = attn(layer, (j * ROWS, (j + 2) * ROWS), info_oth[j], masks, [q_oth], kg, vg, [mlp_oth], w_o2)
                summed = (mine.astype(F32) + to_core(other).astype(F32)).astype(BF16)
                arrived[j] = to_chip(summed)
                after = [summed]
            mine, other = attn(layer, (0, 2 * ROWS), info_own[0], masks, q_own, kg, vg, mlp_own, w_o2, after)
            own = mine.astype(F32) + to_core(other).astype(F32)
            return [(res[j].astype(F32) + own[j * half:(j + 1) * half] + arrived[j].astype(F32) + b_o[layer].astype(F32)
                     + b_down[layer].astype(F32)).astype(BF16) for j in range(2)]

        for layer in range(n_layers):
            res = run_layer(layer, res)

        recv = to_core(pick(res[1], res[0]))
        keep = pick(res[0], res[1])
        return jnp.stack([pick(keep, recv), pick(recv, keep)]).reshape(x_loc.shape)

    return jax.shard_map(local_program, mesh=mesh, in_specs=in_specs, out_specs=P("dp", "tp", None), check_vma=False)
```

```python
import functools

import jax
import jax.numpy as jnp
import numpy as np
from jax import lax
from jax.experimental import pallas as pl
from jax.experimental.pallas import tpu as pltpu
from jax.sharding import PartitionSpec as P


F32, BF16 = jnp.float32, jnp.bfloat16
ROT_DIM = 32
UNIT = ROT_DIM // 2
ROPE_BASE = 10000.0
LN_EPS = 1e-5
LANES = 128
VMEM_LIMIT = 60 * 2**20
ROWS = 512
HEADS = 8
HEAD_DIM = 80
PAIRS = HEADS // 2
ANY = pl.BlockSpec(memory_space=pl.ANY)
VM = pl.BlockSpec(memory_space=pltpu.VMEM)


def packed_units():
    cols = [[None] * 8 for _ in range(5)]
    rest = []
    for p in range(PAIRS):
        base = 2 * (p % 2)
        for e in range(2):
            head = 2 * p + e
            cols[p][base + e] = (head, 0)
            cols[p + 1][base + e] = (head, 1)
    in_first = (6, 4, 2, 0)
    for p in range(PAIRS):
        units = [(2 * p + e, 2 + i) for e in range(2) for i in range(3)]
        rest.append((p, units[:in_first[p]], units[in_first[p]:]))
    for p, first, second in rest:
        for col, units in ((p, first), (p + 1, second)):
            for u in units:
                cols[col][cols[col].index(None)] = u
    return [u for col in cols for u in col]


UNITS = packed_units()
UNIT_ROWS = [h * HEAD_DIM + u * UNIT for h, u in UNITS]


def unit_runs():
    runs, start = [], 0
    for i in range(1, len(UNIT_ROWS) + 1):
        if i == len(UNIT_ROWS) or UNIT_ROWS[i] != UNIT_ROWS[i - 1] + UNIT:
            runs.append((UNIT_ROWS[start], start * UNIT, (i - start) * UNIT))
            start = i
    return runs


def head_masks():
    qk = np.zeros((HEADS, 1, 2 * LANES), np.float32)
    ov = np.zeros((HEADS, 1, 2 * LANES), np.float32)
    for i, (h, _) in enumerate(UNITS):
        lane = i * UNIT - (h // 2) * LANES
        qk[h, 0, lane:lane + UNIT] = 1.0
    for h in range(HEADS):
        lane = h * HEAD_DIM - (h // 2) * LANES
        ov[h, 0, lane:lane + HEAD_DIM] = 1.0
    return qk, ov


def gelu(x):
    return 0.5 * x * (1.0 + jnp.tanh(0.7978845608028654 * (x + 0.044715 * (x * x * x))))


def pre_kernel(nf, layer, n_pair, n_after, info, *refs):
    x_hbm, refs = refs[:2 * n_pair], refs[2 * n_pair:]
    (wq, wk, wv, bqkv_ref, cos_hbm, sin_hbm, wu, bu_ref, wd), refs = refs[:9], refs[9 + n_after:]
    q_out, k_out, v_out, mlp_out = refs[:4]
    x_s, tab_s, y_s, h_s, z_s, u_s, o_s, wp_s, wt_s, x_sem, p_sem, t_sem, h_sem, o_sem = refs[4:]
    R, _ = x_s.shape
    half = ROWS // 2
    nr = R // ROWS
    bf = wt_s.shape[2]
    N = HEADS * HEAD_DIM
    block, core = info[0], info[1]
    row0 = pl.multiple_of(core * half, half)
    row1 = pl.multiple_of((1 - core) * half, half)
    brow = pl.multiple_of(block * ROWS, ROWS)
    xcopies = []
    for p in range(n_pair):
        for s, row in enumerate((row0, row1)):
            xcopies.append(pltpu.make_async_copy(x_hbm[2 * p + s], x_s.at[pl.ds(p * ROWS + row, half)], x_sem.at[2 * p + s]))
    tcopies = [pltpu.make_async_copy(t.at[pl.ds(brow, R)], tab_s.at[s], x_sem.at[2 * n_pair + s]) for s, t in enumerate((cos_hbm, sin_hbm))]
    pcopies = [[pltpu.make_async_copy(w.at[layer, pl.ds(src, n)], wp_s.at[pl.ds(s * N + dst, n)], p_sem.at[s])
                for src, dst, n in unit_runs()] for s, w in enumerate((wq, wk))]
    pcopies.append([pltpu.make_async_copy(wv.at[layer], wp_s.at[pl.ds(2 * N, N)], p_sem.at[2])])
    pwaits = [pltpu.make_async_copy(w.at[layer], wp_s.at[pl.ds(s * N, N)], p_sem.at[s]) for s, w in enumerate((wq, wk, wv))]
    kv_rows = pl.ds(brow, R)
    hcopies = [pltpu.make_async_copy(h_s.at[0], q_out, h_sem.at[0]),
               pltpu.make_async_copy(h_s.at[1], k_out.at[kv_rows], h_sem.at[1]),
               pltpu.make_async_copy(h_s.at[2], v_out.at[kv_rows], h_sem.at[2])]

    def tile_copy(w, t, slot):
        return pltpu.make_async_copy(w.at[layer, :, pl.ds(t * bf, bf)], wt_s.at[slot], t_sem.at[slot])

    def out_copy(t):
        slot = t % 2
        return pltpu.make_async_copy(o_s.at[slot], mlp_out.at[:, pl.ds(t * bf, bf)], o_sem.at[slot])

    def epilogue(r):
        step = 64
        lane = lax.broadcasted_iota(jnp.int32, (step, LANES), 1)
        low, mid = lane < 2 * UNIT, lane < 4 * UNIT
        high = jnp.logical_and(mid, jnp.logical_not(low))
        for rr in range(r * ROWS, (r + 1) * ROWS, step):
            rows = slice(rr, rr + step)
            cos, sin = tab_s[0, rows, :], tab_s[1, rows, :]
            cos_a, cos_ab, cos_b = jnp.where(low, cos, 1.0), jnp.where(mid, cos, 1.0), jnp.where(high, cos, 1.0)
            sin_a, sin_b = jnp.where(low, sin, 0.0), jnp.where(high, sin, 0.0)
            for s in range(3):
                c = [y_s[rows, s * N + i * LANES:s * N + (i + 1) * LANES] + bqkv_ref[:, s * N + i * LANES:s * N + (i + 1) * LANES] for i in range(5)]
                if s < 2:
                    c = [c[0] * cos_a - c[1] * sin_a,
                         c[1] * cos_ab + c[0] * sin_a - c[2] * sin_b,
                         c[2] * cos_ab + c[1] * sin_b - c[3] * sin_a,
                         c[3] * cos_ab + c[2] * sin_a - c[4] * sin_b,
                         c[4] * cos_b + c[3] * sin_b]
                for i in range(5):
                    h_s[s, rows, i * LANES:(i + 1) * LANES] = c[i].astype(BF16)

    def activate(t):
        step = 64
        slot = t % 2
        bias = bu_ref[t].astype(F32)
        for rr in range(0, R, step):
            u_s[t + 1, rr:rr + step, :] = gelu(z_s[slot, rr:rr + step, :] + bias).astype(BF16)

    def slot3(t):
        return t % 3

    for cp in xcopies:
        cp.start()
    tile_copy(wu, 0, 0).start()
    for cp in xcopies:
        cp.wait()

    def up_tile(t, first):
        tile_copy(wu, t, slot3(t)).wait()
        (tile_copy(wu, t + 1, slot3(t + 1)) if t + 1 < nf else tile_copy(wd, 0, slot3(nf))).start()
        for cp in pcopies[t - 1] if 1 <= t <= 3 else tcopies if t == 0 else ():
            cp.start()
        z_s[t % 2] = jnp.dot(x_s[...], wt_s[slot3(t)], preferred_element_type=F32)
        if not first:
            activate(t - 1)

    for t in range(nf):
        up_tile(t, t == 0)
    for cp in pwaits + tcopies:
        cp.wait()
    for r in range(nr):
        rows = slice(r * ROWS, (r + 1) * ROWS)
        y_s[rows, :] = lax.dot_general(x_s[rows, :], wp_s[...], (((1,), (1,)), ((), ())), preferred_element_type=F32)
        if r == 0:
            activate(nf - 1)
        else:
            epilogue(r - 1)

    def down_tile(t, first):
        slot = slot3(t + nf)
        tile_copy(wd, t, slot).wait()
        if t + 1 < nf:
            tile_copy(wd, t + 1, slot3(t + nf + 1)).start()
        if t >= 2:
            out_copy(t - 2).wait()
        u = jnp.concatenate([u_s[f + 1] for f in range(nf)], axis=1)
        o = jnp.dot(u, wt_s[slot], preferred_element_type=F32)
        if first:
            epilogue(nr - 1)
        o_s[t % 2] = o.astype(BF16)
        out_copy(t).start()
        if first:
            for cp in hcopies:
                cp.start()

    for t in range(nf):
        down_tile(t, t == 0)
    out_copy(nf - 2).wait()
    out_copy(nf - 1).wait()
    for cp in hcopies:
        cp.wait()


def pre(layer, info, xs, wq, wk, wv, b_qkv, cos_t, sin_t, w_up, b_up, w_down, kg, vg, after, L, bf=512):
    half, D = xs[0].shape
    n_pair = len(xs) // 2
    R = n_pair * 2 * half
    F = w_up.shape[2]
    nf = F // bf
    N = HEADS * HEAD_DIM
    after = list(after)
    chain = [] if kg is None else [kg, vg]
    n0 = 1 + len(xs) + 9 + len(after)
    return pl.pallas_call(
        functools.partial(pre_kernel, nf, layer, n_pair, len(after) + len(chain)),
        grid_spec=pltpu.PrefetchScalarGridSpec(
            num_scalar_prefetch=1, grid=(),
            in_specs=[ANY] * (len(xs) + 3) + [VM, ANY, ANY, ANY, VM, ANY] + [ANY] * (len(after) + len(chain)),
            out_specs=[ANY] * 4,
            scratch_shapes=[pltpu.VMEM((R, D), BF16), pltpu.VMEM((2, R, LANES), F32), pltpu.VMEM((R, 3 * N), F32),
                            pltpu.VMEM((3, R, N), BF16), pltpu.VMEM((2, R, bf), F32), pltpu.VMEM((nf + 1, R, bf), BF16),
                            pltpu.VMEM((2, R, bf), BF16), pltpu.VMEM((3 * N, D), BF16), pltpu.VMEM((3, D, bf), BF16),
                            pltpu.SemaphoreType.DMA((2 * n_pair + 2,)), pltpu.SemaphoreType.DMA((3,)), pltpu.SemaphoreType.DMA((3,)),
                            pltpu.SemaphoreType.DMA((3,)), pltpu.SemaphoreType.DMA((2,))]),
        out_shape=[jax.ShapeDtypeStruct((R, N), BF16)] + [jax.ShapeDtypeStruct((L, N), BF16)] * 2 + [jax.ShapeDtypeStruct((R, D), BF16)],
        input_output_aliases={} if kg is None else {n0: 1, n0 + 1: 2}, name="pre",
        compiler_params=pltpu.CompilerParams(vmem_limit_bytes=VMEM_LIMIT),
        cost_estimate=pl.CostEstimate(flops=4 * R * D * F + 6 * R * D * N, bytes_accessed=4 * D * F + 4 * R * D, transcendentals=R * F),
    )(info, *xs, wq, wk, wv, b_qkv, cos_t, sin_t, w_up, b_up, w_down, *after, *chain)


def attn_kernel(layer, bases, own, n_blocks, n_after, qm_ref, om_ref, k_hbm, v_hbm, wo_hbm, *refs):
    q_hbm, mlp_hbm, refs = refs[:n_blocks], refs[n_blocks:2 * n_blocks], refs[2 * n_blocks:]
    sum_out, q_s, k_s, v_s, o_s, m_s, w_s, tx_s, rx_s, r_s, in_sem, w_sem, out_sem, send_sem, recv_sem = refs[n_after:]
    R = q_s.shape[0]
    half = ROWS // 2
    n_blk = R // half
    scale = (HEAD_DIM ** -0.5) * 1.4426950408889634
    index = lax.axis_index("tp")
    chip, core = index // 2, lax.rem(index, 2)
    partner = {"tp": 2 * chip + 1 - core}
    barrier = pltpu.get_barrier_semaphore()
    pl.semaphore_signal(barrier, inc=1, device_id=partner, device_id_type=pl.DeviceIdType.MESH)
    cp_w = pltpu.make_async_copy(wo_hbm.at[layer], w_s, w_sem.at[0])
    cp_m = [pltpu.make_async_copy(m, m_s.at[pl.ds(i * ROWS, ROWS)], w_sem.at[1 + i]) for i, m in enumerate(mlp_hbm)]
    cp_q = [pltpu.make_async_copy(q, q_s.at[pl.ds(i * ROWS, ROWS)], in_sem.at[2 + i]) for i, q in enumerate(q_hbm)]

    def run(base):
        seen = pl.ds(0, base + R)
        cp_in = cp_q + [pltpu.make_async_copy(src.at[seen], dst.at[seen], in_sem.at[i])
                        for i, (src, dst) in enumerate(((k_hbm, k_s), (v_hbm, v_s)))]
        for cp in cp_in:
            cp.start()
        o_s[...] = jnp.zeros_like(o_s)
        for cp in cp_in:
            cp.wait()
        cp_w.start()
        for cp in cp_m:
            cp.start()

        def pair(p, carry):
            lanes = pl.ds(pl.multiple_of(p * LANES, LANES), 2 * LANES)
            tasks = [(e, i) for i in range(n_blk) for e in range(2)]

            def scores(e, i):
                n = base + (i + 1) * half
                q = q_s[i * half:(i + 1) * half, lanes] * qm_ref[2 * p + e]
                return lax.dot_general(q, k_s[:n, lanes], (((1,), (1,)), ((), ())), preferred_element_type=F32)

            def rest(s, e, i):
                n = base + (i + 1) * half
                row = lax.broadcasted_iota(jnp.int32, (half, half), 0)
                col = lax.broadcasted_iota(jnp.int32, (half, half), 1)
                diag = jnp.where(row >= col, s[:, n - half:], -1e30)
                s = jnp.concatenate([s[:, :n - half], diag], axis=1) if n > half else diag
                m = jnp.max(s, axis=1, keepdims=True)
                prob = jnp.exp2((s - m) * scale)
                den = jnp.sum(prob, axis=1, keepdims=True)
                o = jnp.dot(prob.astype(BF16), v_s[:n, lanes], preferred_element_type=F32)
                o = jnp.where(om_ref[2 * p + e] > 0.5, o * (1.0 / den), 0.0)
                rows = slice(i * half, (i + 1) * half)
                o_s[rows, lanes] = o_s[rows, lanes] + o.astype(BF16)

            s = scores(*tasks[0])
            for a, t in enumerate(tasks):
                nxt = scores(*tasks[a + 1]) if a + 1 < len(tasks) else None
                rest(s, *t)
                s = nxt
            return carry

        lax.fori_loop(0, PAIRS, pair, 0)

    @pl.when(chip == (0 if own else 1))
    def _():
        run(bases[0])

    @pl.when(chip == (1 if own else 0))
    def _():
        run(bases[1])

    cp_w.wait()
    for cp in cp_m:
        cp.wait()
    pl.semaphore_wait(barrier, 1)

    def partial(block, which):
        rows = pl.ds(pl.multiple_of(block * ROWS + which * half, half), half)
        return jnp.dot(o_s[rows, :], w_s[...], preferred_element_type=F32) + m_s[rows, :].astype(F32)

    sends = []
    for b in range(n_blocks):
        tx_s[b] = partial(b, 1 - core).astype(BF16)
        cp = pltpu.make_async_remote_copy(src_ref=tx_s.at[b], dst_ref=rx_s.at[b], send_sem=send_sem.at[b], recv_sem=recv_sem.at[b],
                                          device_id=partner, device_id_type=pl.DeviceIdType.MESH)
        cp.start()
        sends.append(cp)
    outs = []
    for b in range(n_blocks):
        r_s[b] = partial(b, core)
    for b in range(n_blocks):
        sends[b].wait()
        tx_s[b] = (r_s[b] + rx_s[b].astype(F32)).astype(BF16)
        cp = pltpu.make_async_copy(tx_s.at[b], sum_out.at[pl.ds(b * half, half)], out_sem.at[b])
        cp.start()
        outs.append(cp)
    for cp in outs:
        cp.wait()


def attn(layer, bases, own, call_id, masks, q, kg, vg, mlp_part, w_o, after=()):
    n_blocks, N = len(q), q[0].shape[1]
    R = n_blocks * ROWS
    half = ROWS // 2
    L = kg.shape[0]
    D = w_o.shape[2]
    after = list(after)
    dma = pltpu.SemaphoreType.DMA
    return pl.pallas_call(
        functools.partial(attn_kernel, layer, bases, own, n_blocks, len(after)),
        in_specs=[VM, VM] + [ANY] * (3 + 2 * n_blocks + len(after)),
        out_specs=ANY,
        scratch_shapes=[pltpu.VMEM((R, N), BF16), pltpu.VMEM((L, N), BF16), pltpu.VMEM((L, N), BF16), pltpu.VMEM((R, N), BF16),
                        pltpu.VMEM((R, D), BF16), pltpu.VMEM((N, D), BF16), pltpu.VMEM((n_blocks, half, D), BF16),
                        pltpu.VMEM((n_blocks, half, D), BF16), pltpu.VMEM((n_blocks, half, D), F32),
                        dma((2 + n_blocks,)), dma((1 + n_blocks,)), dma((n_blocks,)), dma((n_blocks,)), dma((n_blocks,))],
        out_shape=jax.ShapeDtypeStruct((R // 2, D), BF16), name="attn",
        compiler_params=pltpu.CompilerParams(vmem_limit_bytes=VMEM_LIMIT, collective_id=call_id, has_side_effects=True),
        cost_estimate=pl.CostEstimate(flops=4 * HEADS * R * (L // 2) * 128 + 2 * R * D * N, bytes_accessed=4 * L * N, transcendentals=HEADS * R * L // 2),
    )(*masks, kg, vg, w_o, *q, *mlp_part, *after)


def rotary_tables(seq_len):
    unit = jnp.arange(LANES) % UNIT
    inv_freq = 1.0 / (ROPE_BASE ** (unit.astype(F32) * (2.0 / ROT_DIM)))
    angles = jnp.arange(seq_len, dtype=F32)[:, None] * inv_freq[None, :]
    return jnp.cos(angles), jnp.sin(angles)


def layer_norm(x_f32, gain, bias):
    mean = jnp.mean(x_f32, axis=-1, keepdims=True)
    centered = x_f32 - mean
    variance = jnp.mean(centered * centered, axis=-1, keepdims=True)
    return (centered * lax.rsqrt(variance + LN_EPS) * gain.astype(F32) + bias.astype(F32)).astype(BF16)


def solution(mesh):
    head_spec = P(None, None, "tp", None)
    head_bias_spec = P(None, "tp", None)
    in_specs = (P("dp", "tp", None), P(), P(), head_spec, head_bias_spec, head_spec, head_bias_spec, head_spec, head_bias_spec,
                P(None, "tp", None, None), P(), P(None, None, "tp"), P(None, "tp"), P(None, "tp", None), P())
    across = [(0, 2), (1, 3), (2, 0), (3, 1)]
    partner = [(0, 1), (1, 0), (2, 3), (3, 2)]

    def to_chip(a):
        return lax.ppermute(a, "tp", across)

    def to_core(a):
        return lax.ppermute(a, "tp", partner)

    def behind(a, done):
        return lax.optimization_barrier((a, done))[0]

    def local_program(x_loc, ln_gain, ln_bias, w_q, b_q, w_k, b_k, w_v, b_v, w_o, b_o, w_up, b_up, w_down, b_down):
        n_layers, d_model, heads, head_dim = w_q.shape
        width = heads * head_dim
        half = x_loc.shape[1] // 2
        seq_len = 4 * x_loc.shape[1]
        index = lax.axis_index("tp")
        chip, core = index // 2, index % 2
        cos_t, sin_t = rotary_tables(seq_len)
        qk_mask, out_mask = head_masks()
        masks = (jnp.asarray(qk_mask, BF16), jnp.asarray(out_mask, F32))
        w_o2 = w_o.reshape(n_layers, width, d_model)
        w_qt, w_kt, w_vt = (jnp.transpose(w, (0, 2, 3, 1)).reshape(n_layers, width, d_model) for w in (w_q, w_k, w_v))

        def pick(first, second):
            return jnp.where(core == 0, first, second)

        def packed(bias):
            flat = bias.astype(F32).reshape(width)
            return jnp.concatenate([flat[r:r + UNIT] for r in UNIT_ROWS])

        x_halves = x_loc[0, :half], x_loc[0, half:]
        keep = pick(*x_halves)
        recv = to_core(pick(x_halves[1], x_halves[0]))
        res = [pick(keep, recv), pick(recv, keep)]
        info_own = [jnp.stack([2 * chip + j, core]).astype(jnp.int32) for j in range(2)]
        info_oth = [jnp.stack([2 * (1 - chip) + j, core]).astype(jnp.int32) for j in range(2)]

        def run_layer(layer, res):
            b_qkv = jnp.concatenate([packed(b_q[layer]), packed(b_k[layer]), b_v[layer].astype(F32).reshape(width)])[None]
            b_up3 = b_up[layer].reshape(-1, 1, 512)
            norm = [layer_norm(res[j].astype(F32), ln_gain[layer], ln_bias[layer]) for j in range(2)]
            far = [None, None]
            for j in range(2):
                far[j] = to_chip(norm[j])
            near = [to_core(norm[j]) for j in range(2)]

            def project(info, a, b, kg, vg, after):
                return pre(layer, info, [a, b], w_qt, w_kt, w_vt, b_qkv, cos_t, sin_t, w_up, b_up3, w_down, kg, vg, after, seq_len)

            q_own, mlp_own, relay = [None, None], [None, None], [None, None]
            kg = vg = None
            after = []
            for j in range(2):
                q_own[j], kg, vg, mlp_own[j] = project(info_own[j], norm[j], near[j], kg, vg, after)
                far[j] = behind(far[j], mlp_own[j])
                relay[j] = to_core(far[j])
                after = [far[j]]
            arrived = [None, None]
            for j in range(2):
                q_oth, kg, vg, mlp_oth = project(info_oth[j], far[j], relay[j], kg, vg, after)
                summed = attn(layer, (j * ROWS, (j + 2) * ROWS), False, 3 * layer + j, masks, [q_oth], kg, vg, [mlp_oth], w_o2)
                arrived[j] = to_chip(summed)
                after = [summed]
            own = attn(layer, (0, 2 * ROWS), True, 3 * layer + 2, masks, q_own, kg, vg, mlp_own, w_o2, after)
            return [(res[j].astype(F32) + own[j * half:(j + 1) * half].astype(F32) + arrived[j].astype(F32) + b_o[layer].astype(F32)
                     + b_down[layer].astype(F32)).astype(BF16) for j in range(2)]

        for layer in range(n_layers):
            res = run_layer(layer, res)

        recv = to_core(pick(res[1], res[0]))
        keep = pick(res[0], res[1])
        return jnp.stack([pick(keep, recv), pick(recv, keep)]).reshape(x_loc.shape)

    return jax.shard_map(local_program, mesh=mesh, in_specs=in_specs, out_specs=P("dp", "tp", None), check_vma=False)
```

```python
import functools

import jax
import jax.numpy as jnp
import numpy as np
from jax import lax
from jax.experimental import pallas as pl
from jax.experimental.pallas import tpu as pltpu
from jax.sharding import PartitionSpec as P


F32, BF16 = jnp.float32, jnp.bfloat16
ROT_DIM = 32
UNIT = ROT_DIM // 2
ROPE_BASE = 10000.0
LN_EPS = 1e-5
LANES = 128
VMEM_LIMIT = 60 * 2**20
ROWS = 512
HEADS = 8
HEAD_DIM = 80
PAIRS = HEADS // 2
ANY = pl.BlockSpec(memory_space=pl.ANY)
VM = pl.BlockSpec(memory_space=pltpu.VMEM)


def packed_units():
    cols = [[None] * 8 for _ in range(5)]
    rest = []
    for p in range(PAIRS):
        base = 2 * (p % 2)
        for e in range(2):
            head = 2 * p + e
            cols[p][base + e] = (head, 0)
            cols[p + 1][base + e] = (head, 1)
    in_first = (6, 4, 2, 0)
    for p in range(PAIRS):
        units = [(2 * p + e, 2 + i) for e in range(2) for i in range(3)]
        rest.append((p, units[:in_first[p]], units[in_first[p]:]))
    for p, first, second in rest:
        for col, units in ((p, first), (p + 1, second)):
            for u in units:
                cols[col][cols[col].index(None)] = u
    return [u for col in cols for u in col]


UNITS = packed_units()
UNIT_ROWS = [h * HEAD_DIM + u * UNIT for h, u in UNITS]


def unit_runs():
    runs, start = [], 0
    for i in range(1, len(UNIT_ROWS) + 1):
        if i == len(UNIT_ROWS) or UNIT_ROWS[i] != UNIT_ROWS[i - 1] + UNIT:
            runs.append((UNIT_ROWS[start], start * UNIT, (i - start) * UNIT))
            start = i
    return runs


def head_masks():
    qk = np.zeros((HEADS, 1, 2 * LANES), np.float32)
    ov = np.zeros((HEADS, 1, 2 * LANES), np.float32)
    for i, (h, _) in enumerate(UNITS):
        lane = i * UNIT - (h // 2) * LANES
        qk[h, 0, lane:lane + UNIT] = 1.0
    for h in range(HEADS):
        lane = h * HEAD_DIM - (h // 2) * LANES
        ov[h, 0, lane:lane + HEAD_DIM] = 1.0
    return qk, ov


def gelu(x):
    return 0.5 * x * (1.0 + jnp.tanh(0.7978845608028654 * (x + 0.044715 * (x * x * x))))


def pre_kernel(nf, layer, n_pair, n_after, info, *refs):
    x_hbm, refs = refs[:2 * n_pair], refs[2 * n_pair:]
    (wq, wk, wv, bqkv_ref, cos_hbm, sin_hbm, wu, bu_ref, wd), refs = refs[:9], refs[9 + n_after:]
    q_out, k_out, v_out, mlp_out = refs[:4]
    x_s, tab_s, y_s, h_s, z_s, u_s, o_s, wp_s, wt_s, x_sem, p_sem, t_sem, h_sem, o_sem = refs[4:]
    R, _ = x_s.shape
    half = ROWS // 2
    nr = R // ROWS
    bf = wt_s.shape[2]
    N = HEADS * HEAD_DIM
    block, core = info[0], info[1]
    row0 = pl.multiple_of(core * half, half)
    row1 = pl.multiple_of((1 - core) * half, half)
    brow = pl.multiple_of(block * ROWS, ROWS)
    xcopies = []
    for p in range(n_pair):
        for s, row in enumerate((row0, row1)):
            xcopies.append(pltpu.make_async_copy(x_hbm[2 * p + s], x_s.at[pl.ds(p * ROWS + row, half)], x_sem.at[2 * p + s]))
    tcopies = [pltpu.make_async_copy(t.at[pl.ds(brow, R)], tab_s.at[s], x_sem.at[2 * n_pair + s]) for s, t in enumerate((cos_hbm, sin_hbm))]
    pcopies = []
    for s, w in enumerate((wq, wk)):
        for src, dst, n in unit_runs():
            pcopies.append(pltpu.make_async_copy(w.at[layer, pl.ds(src, n)], wp_s.at[pl.ds(s * N + dst, n)], p_sem.at[s]))
    pcopies.append(pltpu.make_async_copy(wv.at[layer], wp_s.at[pl.ds(2 * N, N)], p_sem.at[2]))
    pwaits = [pltpu.make_async_copy(w.at[layer], wp_s.at[pl.ds(s * N, N)], p_sem.at[s]) for s, w in enumerate((wq, wk, wv))]
    kv_rows = pl.ds(brow, R)
    hcopies = [pltpu.make_async_copy(h_s.at[0], q_out, h_sem.at[0]),
               pltpu.make_async_copy(h_s.at[1], k_out.at[kv_rows], h_sem.at[1]),
               pltpu.make_async_copy(h_s.at[2], v_out.at[kv_rows], h_sem.at[2])]

    def tile_copy(w, t, slot):
        return pltpu.make_async_copy(w.at[layer, :, pl.ds(pl.multiple_of(t * bf, bf), bf)], wt_s.at[slot], t_sem.at[slot])

    def out_copy(t):
        slot = lax.rem(t, 2)
        return pltpu.make_async_copy(o_s.at[slot], mlp_out.at[:, pl.ds(pl.multiple_of(t * bf, bf), bf)], o_sem.at[slot])

    def epilogue(r):
        step = 64
        lane = lax.broadcasted_iota(jnp.int32, (step, LANES), 1)
        low, mid = lane < 2 * UNIT, lane < 4 * UNIT
        high = jnp.logical_and(mid, jnp.logical_not(low))
        for rr in range(r * ROWS, (r + 1) * ROWS, step):
            rows = slice(rr, rr + step)
            cos, sin = tab_s[0, rows, :], tab_s[1, rows, :]
            cos_a, cos_ab, cos_b = jnp.where(low, cos, 1.0), jnp.where(mid, cos, 1.0), jnp.where(high, cos, 1.0)
            sin_a, sin_b = jnp.where(low, sin, 0.0), jnp.where(high, sin, 0.0)
            for s in range(3):
                c = [y_s[rows, s * N + i * LANES:s * N + (i + 1) * LANES] + bqkv_ref[:, s * N + i * LANES:s * N + (i + 1) * LANES] for i in range(5)]
                if s < 2:
                    c = [c[0] * cos_a - c[1] * sin_a,
                         c[1] * cos_ab + c[0] * sin_a - c[2] * sin_b,
                         c[2] * cos_ab + c[1] * sin_b - c[3] * sin_a,
                         c[3] * cos_ab + c[2] * sin_a - c[4] * sin_b,
                         c[4] * cos_b + c[3] * sin_b]
                for i in range(5):
                    h_s[s, rows, i * LANES:(i + 1) * LANES] = c[i].astype(BF16)

    def activate(t):
        step = 64
        slot = lax.rem(t, 2)
        bias = bu_ref[t].astype(F32)
        for rr in range(0, R, step):
            u_s[t + 1, rr:rr + step, :] = gelu(z_s[slot, rr:rr + step, :] + bias).astype(BF16)

    def slot3(t):
        return lax.rem(t, 3)

    for cp in xcopies:
        cp.start()
    tile_copy(wu, 0, 0).start()
    tile_copy(wu, 1, 1).start()
    for cp in pcopies + tcopies:
        cp.start()
    for cp in xcopies:
        cp.wait()

    def up_tile(t, first):
        tile_copy(wu, t, slot3(t)).wait()
        if isinstance(t, int):
            (tile_copy(wu, t + 2, slot3(t + 2)) if t + 2 < nf else tile_copy(wd, t + 2 - nf, slot3(t + 2))).start()
        else:
            @pl.when(t + 2 < nf)
            def _():
                tile_copy(wu, t + 2, slot3(t + 2)).start()

            @pl.when(t + 2 >= nf)
            def _():
                tile_copy(wd, t + 2 - nf, slot3(t + 2)).start()
        z_s[lax.rem(t, 2)] = jnp.dot(x_s[...], wt_s[slot3(t)], preferred_element_type=F32)
        if not first:
            activate(t - 1)

    if nr == 1:
        for t in range(nf):
            up_tile(t, t == 0)
    else:
        up_tile(0, True)
        lax.fori_loop(1, nf, lambda t, c: (up_tile(t, False), c)[1], 0)
    for cp in pwaits + tcopies:
        cp.wait()
    for r in range(nr):
        rows = slice(r * ROWS, (r + 1) * ROWS)
        y_s[rows, :] = lax.dot_general(x_s[rows, :], wp_s[...], (((1,), (1,)), ((), ())), preferred_element_type=F32)
        if r == 0:
            activate(nf - 1)
        else:
            epilogue(r - 1)

    def down_tile(t, first):
        slot = slot3(t + nf)
        tile_copy(wd, t, slot).wait()
        if isinstance(t, int):
            if t + 2 < nf:
                tile_copy(wd, t + 2, slot3(t + nf + 2)).start()
            if t >= 2:
                out_copy(t - 2).wait()
        else:
            @pl.when(t + 2 < nf)
            def _():
                tile_copy(wd, t + 2, slot3(t + nf + 2)).start()

            @pl.when(t >= 2)
            def _():
                out_copy(t - 2).wait()
        u = jnp.concatenate([u_s[f + 1] for f in range(nf)], axis=1)
        o = jnp.dot(u, wt_s[slot], preferred_element_type=F32)
        if first:
            epilogue(nr - 1)
        o_s[lax.rem(t, 2)] = o.astype(BF16)
        out_copy(t).start()
        if first:
            for cp in hcopies:
                cp.start()

    if nr == 1:
        for t in range(nf):
            down_tile(t, t == 0)
    else:
        down_tile(0, True)
        lax.fori_loop(1, nf, lambda t, c: (down_tile(t, False), c)[1], 0)
    out_copy(nf - 2).wait()
    out_copy(nf - 1).wait()
    for cp in hcopies:
        cp.wait()


def pre(layer, info, xs, wq, wk, wv, b_qkv, cos_t, sin_t, w_up, b_up, w_down, kg, vg, after, L, bf=512):
    half, D = xs[0].shape
    n_pair = len(xs) // 2
    R = n_pair * 2 * half
    F = w_up.shape[2]
    nf = F // bf
    N = HEADS * HEAD_DIM
    after = list(after)
    chain = [] if kg is None else [kg, vg]
    n0 = 1 + len(xs) + 9 + len(after)
    return pl.pallas_call(
        functools.partial(pre_kernel, nf, layer, n_pair, len(after) + len(chain)),
        grid_spec=pltpu.PrefetchScalarGridSpec(
            num_scalar_prefetch=1, grid=(),
            in_specs=[ANY] * (len(xs) + 3) + [VM, ANY, ANY, ANY, VM, ANY] + [ANY] * (len(after) + len(chain)),
            out_specs=[ANY] * 4,
            scratch_shapes=[pltpu.VMEM((R, D), BF16), pltpu.VMEM((2, R, LANES), F32), pltpu.VMEM((R, 3 * N), F32),
                            pltpu.VMEM((3, R, N), BF16), pltpu.VMEM((2, R, bf), F32), pltpu.VMEM((nf + 1, R, bf), BF16),
                            pltpu.VMEM((2, R, bf), BF16), pltpu.VMEM((3 * N, D), BF16), pltpu.VMEM((3, D, bf), BF16),
                            pltpu.SemaphoreType.DMA((2 * n_pair + 2,)), pltpu.SemaphoreType.DMA((3,)), pltpu.SemaphoreType.DMA((3,)),
                            pltpu.SemaphoreType.DMA((3,)), pltpu.SemaphoreType.DMA((2,))]),
        out_shape=[jax.ShapeDtypeStruct((R, N), BF16)] + [jax.ShapeDtypeStruct((L, N), BF16)] * 2 + [jax.ShapeDtypeStruct((R, D), BF16)],
        input_output_aliases={} if kg is None else {n0: 1, n0 + 1: 2}, name="pre",
        compiler_params=pltpu.CompilerParams(vmem_limit_bytes=VMEM_LIMIT),
        cost_estimate=pl.CostEstimate(flops=4 * R * D * F + 6 * R * D * N, bytes_accessed=4 * D * F + 4 * R * D, transcendentals=R * F),
    )(info, *xs, wq, wk, wv, b_qkv, cos_t, sin_t, w_up, b_up, w_down, *after, *chain)


def attn_kernel(layer, bases, own, n_blocks, n_after, qm_ref, om_ref, k_hbm, v_hbm, wo_hbm, *refs):
    q_hbm, mlp_hbm, refs = refs[:n_blocks], refs[n_blocks:2 * n_blocks], refs[2 * n_blocks:]
    sum_out, q_s, k_s, v_s, o_s, m_s, w_s, tx_s, rx_s, r_s, in_sem, w_sem, out_sem, send_sem, recv_sem = refs[n_after:]
    R = q_s.shape[0]
    half = ROWS // 2
    n_blk = R // half
    scale = (HEAD_DIM ** -0.5) * 1.4426950408889634
    index = lax.axis_index("tp")
    chip, core = index // 2, lax.rem(index, 2)
    partner = {"tp": 2 * chip + 1 - core}
    barrier = pltpu.get_barrier_semaphore()
    pl.semaphore_signal(barrier, inc=1, device_id=partner, device_id_type=pl.DeviceIdType.MESH)
    cp_w = pltpu.make_async_copy(wo_hbm.at[layer], w_s, w_sem.at[0])
    cp_m = [pltpu.make_async_copy(m, m_s.at[pl.ds(i * ROWS, ROWS)], w_sem.at[1 + i]) for i, m in enumerate(mlp_hbm)]
    cp_q = [pltpu.make_async_copy(q, q_s.at[pl.ds(i * ROWS, ROWS)], in_sem.at[2 + i]) for i, q in enumerate(q_hbm)]

    def run(base):
        seen = pl.ds(0, base + R)
        cp_in = cp_q + [pltpu.make_async_copy(src.at[seen], dst.at[seen], in_sem.at[i])
                        for i, (src, dst) in enumerate(((k_hbm, k_s), (v_hbm, v_s)))]
        for cp in cp_in:
            cp.start()
        o_s[...] = jnp.zeros_like(o_s)
        for cp in cp_in:
            cp.wait()
        cp_w.start()
        for cp in cp_m:
            cp.start()

        def pair(p, carry):
            lanes = pl.ds(pl.multiple_of(p * LANES, LANES), 2 * LANES)
            tasks = [(e, i) for i in range(n_blk) for e in range(2)]

            def scores(e, i):
                n = base + (i + 1) * half
                q = q_s[i * half:(i + 1) * half, lanes] * qm_ref[2 * p + e]
                return lax.dot_general(q, k_s[:n, lanes], (((1,), (1,)), ((), ())), preferred_element_type=F32)

            def rest(s, e, i):
                n = base + (i + 1) * half
                row = lax.broadcasted_iota(jnp.int32, (half, half), 0)
                col = lax.broadcasted_iota(jnp.int32, (half, half), 1)
                diag = jnp.where(row >= col, s[:, n - half:], -1e30)
                s = jnp.concatenate([s[:, :n - half], diag], axis=1) if n > half else diag
                m = jnp.max(s, axis=1, keepdims=True)
                prob = jnp.exp2((s - m) * scale)
                den = jnp.sum(prob, axis=1, keepdims=True)
                o = jnp.dot(prob.astype(BF16), v_s[:n, lanes], preferred_element_type=F32)
                o = jnp.where(om_ref[2 * p + e] > 0.5, o * (1.0 / den), 0.0)
                rows = slice(i * half, (i + 1) * half)
                o_s[rows, lanes] = o_s[rows, lanes] + o.astype(BF16)

            s = scores(*tasks[0])
            for a, t in enumerate(tasks):
                nxt = scores(*tasks[a + 1]) if a + 1 < len(tasks) else None
                rest(s, *t)
                s = nxt
            return carry

        lax.fori_loop(0, PAIRS, pair, 0)

    @pl.when(chip == (0 if own else 1))
    def _():
        run(bases[0])

    @pl.when(chip == (1 if own else 0))
    def _():
        run(bases[1])

    cp_w.wait()
    for cp in cp_m:
        cp.wait()
    pl.semaphore_wait(barrier, 1)

    def partial(block, which):
        rows = pl.ds(pl.multiple_of(block * ROWS + which * half, half), half)
        return jnp.dot(o_s[rows, :], w_s[...], preferred_element_type=F32) + m_s[rows, :].astype(F32)

    sends = []
    for b in range(n_blocks):
        tx_s[b] = partial(b, 1 - core).astype(BF16)
        cp = pltpu.make_async_remote_copy(src_ref=tx_s.at[b], dst_ref=rx_s.at[b], send_sem=send_sem.at[b], recv_sem=recv_sem.at[b],
                                          device_id=partner, device_id_type=pl.DeviceIdType.MESH)
        cp.start()
        sends.append(cp)
    outs = []
    for b in range(n_blocks):
        r_s[b] = partial(b, core)
    for b in range(n_blocks):
        sends[b].wait()
        tx_s[b] = (r_s[b] + rx_s[b].astype(F32)).astype(BF16)
        cp = pltpu.make_async_copy(tx_s.at[b], sum_out.at[pl.ds(b * half, half)], out_sem.at[b])
        cp.start()
        outs.append(cp)
    for cp in outs:
        cp.wait()


def attn(layer, bases, own, call_id, masks, q, kg, vg, mlp_part, w_o, after=()):
    n_blocks, N = len(q), q[0].shape[1]
    R = n_blocks * ROWS
    half = ROWS // 2
    L = kg.shape[0]
    D = w_o.shape[2]
    after = list(after)
    dma = pltpu.SemaphoreType.DMA
    return pl.pallas_call(
        functools.partial(attn_kernel, layer, bases, own, n_blocks, len(after)),
        in_specs=[VM, VM] + [ANY] * (3 + 2 * n_blocks + len(after)),
        out_specs=ANY,
        scratch_shapes=[pltpu.VMEM((R, N), BF16), pltpu.VMEM((L, N), BF16), pltpu.VMEM((L, N), BF16), pltpu.VMEM((R, N), BF16),
                        pltpu.VMEM((R, D), BF16), pltpu.VMEM((N, D), BF16), pltpu.VMEM((n_blocks, half, D), BF16),
                        pltpu.VMEM((n_blocks, half, D), BF16), pltpu.VMEM((n_blocks, half, D), F32),
                        dma((2 + n_blocks,)), dma((1 + n_blocks,)), dma((n_blocks,)), dma((n_blocks,)), dma((n_blocks,))],
        out_shape=jax.ShapeDtypeStruct((R // 2, D), BF16), name="attn",
        compiler_params=pltpu.CompilerParams(vmem_limit_bytes=VMEM_LIMIT, collective_id=call_id, has_side_effects=True),
        cost_estimate=pl.CostEstimate(flops=4 * HEADS * R * (L // 2) * 128 + 2 * R * D * N, bytes_accessed=4 * L * N, transcendentals=HEADS * R * L // 2),
    )(*masks, kg, vg, w_o, *q, *mlp_part, *after)


def rotary_tables(seq_len):
    unit = jnp.arange(LANES) % UNIT
    inv_freq = 1.0 / (ROPE_BASE ** (unit.astype(F32) * (2.0 / ROT_DIM)))
    angles = jnp.arange(seq_len, dtype=F32)[:, None] * inv_freq[None, :]
    return jnp.cos(angles), jnp.sin(angles)


def layer_norm(x_f32, gain, bias):
    mean = jnp.mean(x_f32, axis=-1, keepdims=True)
    centered = x_f32 - mean
    variance = jnp.mean(centered * centered, axis=-1, keepdims=True)
    return (centered * lax.rsqrt(variance + LN_EPS) * gain.astype(F32) + bias.astype(F32)).astype(BF16)


def solution(mesh):
    head_spec = P(None, None, "tp", None)
    head_bias_spec = P(None, "tp", None)
    in_specs = (P("dp", "tp", None), P(), P(), head_spec, head_bias_spec, head_spec, head_bias_spec, head_spec, head_bias_spec,
                P(None, "tp", None, None), P(), P(None, None, "tp"), P(None, "tp"), P(None, "tp", None), P())
    across = [(0, 2), (1, 3), (2, 0), (3, 1)]
    partner = [(0, 1), (1, 0), (2, 3), (3, 2)]

    def to_chip(a):
        return lax.ppermute(a, "tp", across)

    def to_core(a):
        return lax.ppermute(a, "tp", partner)

    def behind(a, done):
        return lax.optimization_barrier((a, done))[0]

    def local_program(x_loc, ln_gain, ln_bias, w_q, b_q, w_k, b_k, w_v, b_v, w_o, b_o, w_up, b_up, w_down, b_down):
        n_layers, d_model, heads, head_dim = w_q.shape
        width = heads * head_dim
        half = x_loc.shape[1] // 2
        seq_len = 4 * x_loc.shape[1]
        index = lax.axis_index("tp")
        chip, core = index // 2, index % 2
        cos_t, sin_t = rotary_tables(seq_len)
        qk_mask, out_mask = head_masks()
        masks = (jnp.asarray(qk_mask, BF16), jnp.asarray(out_mask, F32))
        w_o2 = w_o.reshape(n_layers, width, d_model)
        w_qt, w_kt, w_vt = (jnp.transpose(w, (0, 2, 3, 1)).reshape(n_layers, width, d_model) for w in (w_q, w_k, w_v))

        def pick(first, second):
            return jnp.where(core == 0, first, second)

        def packed(bias):
            flat = bias.astype(F32).reshape(width)
            return jnp.concatenate([flat[r:r + UNIT] for r in UNIT_ROWS])

        x_halves = x_loc[0, :half], x_loc[0, half:]
        keep = pick(*x_halves)
        recv = to_core(pick(x_halves[1], x_halves[0]))
        res = [pick(keep, recv), pick(recv, keep)]
        info_own = [jnp.stack([2 * chip + j, core]).astype(jnp.int32) for j in range(2)]
        info_oth = [jnp.stack([2 * (1 - chip) + j, core]).astype(jnp.int32) for j in range(2)]

        def run_layer(layer, res):
            b_qkv = jnp.concatenate([packed(b_q[layer]), packed(b_k[layer]), b_v[layer].astype(F32).reshape(width)])[None]
            b_up3 = b_up[layer].reshape(-1, 1, 512)
            norm = [layer_norm(res[j].astype(F32), ln_gain[layer], ln_bias[layer]) for j in range(2)]
            far = [None, None]
            for j in range(2):
                far[j] = to_chip(norm[j])
            near = [to_core(norm[j]) for j in range(2)]

            def project(info, a, b, kg, vg, after):
                return pre(layer, info, [a, b], w_qt, w_kt, w_vt, b_qkv, cos_t, sin_t, w_up, b_up3, w_down, kg, vg, after, seq_len)

            q_own, mlp_own, relay = [None, None], [None, None], [None, None]
            kg = vg = None
            after = []
            for j in range(2):
                q_own[j], kg, vg, mlp_own[j] = project(info_own[j], norm[j], near[j], kg, vg, after)
                far[j] = behind(far[j], mlp_own[j])
                relay[j] = to_core(far[j])
                after = [far[j]]
            arrived = [None, None]
            for j in range(2):
                q_oth, kg, vg, mlp_oth = project(info_oth[j], far[j], relay[j], kg, vg, after)
                summed = attn(layer, (j * ROWS, (j + 2) * ROWS), False, 3 * layer + j, masks, [q_oth], kg, vg, [mlp_oth], w_o2)
                arrived[j] = to_chip(summed)
                after = [summed]
            own = attn(layer, (0, 2 * ROWS), True, 3 * layer + 2, masks, q_own, kg, vg, mlp_own, w_o2, after)
            return [(res[j].astype(F32) + own[j * half:(j + 1) * half].astype(F32) + arrived[j].astype(F32) + b_o[layer].astype(F32)
                     + b_down[layer].astype(F32)).astype(BF16) for j in range(2)]

        for layer in range(n_layers):
            res = run_layer(layer, res)

        recv = to_core(pick(res[1], res[0]))
        keep = pick(res[0], res[1])
        return jnp.stack([pick(keep, recv), pick(recv, keep)]).reshape(x_loc.shape)

    return jax.shard_map(local_program, mesh=mesh, in_specs=in_specs, out_specs=P("dp", "tp", None), check_vma=False)
```
